32 devices in a mesh: section: 4 (over x, core), dp: 8 (over z, y).
Axes of the slice: x: 2, y: 2, z: 4, core: 2. Of those that a mesh axis runs over, the one named last changes fastest.
Arguments:
- hidden_in: bfloat16 [8, 512, 2048], P(None, 'dp'), may hold values from -8 to 8
- norm_gain: bfloat16 [4, 2048], P('section'), may hold values from 0.099609375 to 1.8984375
- router_weight: bfloat16 [4, 2048, 60], P('section'), may hold values from -1 to 1
- expert_scale: bfloat16 [4, 60, 2048], P('section'), may hold values from 1 to 16
- mix_weight: bfloat16 [4, 2048, 2048], P('section'), may hold values from -0.125 to 0.125
- routes: int32 [4, 8, 512, 4], P('section', None, 'dp'), may hold values from 0 to 59, as said below
Outputs:
- hidden_out: bfloat16 [8, 512, 2048], P('section', 'dp')
- balance_loss: float32 [4], P('section')
The draws below stay inside these ranges and needn't reach their ends.
Inputs may be any that keep to these rules, and one draw needn't show every extreme that they name: `routes`: the 4 ids of a token in a layer are distinct.
All inputs are finite; a program needn't handle non-finite values.
Results may differ from the reference program's by a relative error of at most 0.01.
The reference program's roundings to bfloat16 on the way count: a program that leaves them out, or rounds other values in their place, can miss the bound.
Values may be sent and summed in bfloat16 or wider, within the bound.
A program may use at most 64 MiB of HBM per device.

```python
import math
import jax
import jax.numpy as jnp
from jax import lax

D = 2048
E = 60
K = 4
M = 8
TOK_DEV = 64
TOK_MB = 512
LAYERS = 4


def common_direction(key):
    signs = jax.random.randint(jax.random.fold_in(key, 7001), (D,), 0, 2)
    return signs.astype(jnp.float32) * 2.0 - 1.0


def draw_hidden_in(key, part):
    direction = common_direction(key)
    noise_key = jax.random.fold_in(key, 11)
    noise = jnp.clip(jax.random.normal(noise_key, (M, TOK_MB, D), jnp.float32), -6.0, 6.0)
    strength = jnp.ones((TOK_MB,), jnp.float32)
    values = noise + strength[None, :, None] * direction[None, None, :]
    return values.astype(jnp.bfloat16)


def draw_router_weight(key, part):
    direction = common_direction(key)
    noise = jnp.clip(jax.random.normal(jax.random.fold_in(key, 12), (LAYERS, D, E), jnp.float32), -6.0, 6.0)
    noise = noise / jnp.sqrt(jnp.float32(D))
    tilt = 2.0 * jnp.arange(E).astype(jnp.float32) / jnp.float32(E - 1) - 1.0
    lean = 4.0 * tilt[None, None, :] * direction[None, :, None] / jnp.float32(D)
    return (noise + lean).astype(jnp.bfloat16)


def draw_routes(key, part):
    shard_count = TOK_MB // TOK_DEV
    shard = jnp.arange(TOK_MB, dtype=jnp.int32) // TOK_DEV
    target = shard * (E - 1) // max(shard_count - 1, 1)
    expert_ids = jnp.arange(E, dtype=jnp.int32)
    distance = jnp.abs(expert_ids[None, :] - target[:, None])
    noise = jax.random.randint(jax.random.fold_in(key, 13), (LAYERS, M, TOK_MB, E), 0, 40)
    scores = (noise - distance[None, None, :, :]) * 64 + expert_ids[None, None, None, :]
    picked = lax.top_k(scores, K)[1]
    return picked.astype(jnp.int32)


def level_of(stream_key, dims, cuts, low, high):
    level, own = 1.0, jax.random.fold_in(stream_key, 6)
    for axis_at, shards_of in cuts:
        steps = jnp.exp(jax.random.uniform(jax.random.fold_in(own, axis_at), (shards_of,), jnp.float32, low / len(cuts), high / len(cuts)))
        level = level * jnp.repeat(steps, dims[axis_at] // shards_of).reshape([-1 if axis == axis_at else 1 for axis in range(len(dims))])
    return level


def bell_draw(key, shape, spread, most, shards=(), kind=jnp.bfloat16):
    gain = level_of(key, shape, shards, -0.22, 0.18) if shards else 1.0
    values = jax.random.normal(key, shape, jnp.float32) * spread * gain
    return jnp.minimum(jnp.maximum(values, -most), most).astype(kind)


def setup_inputs(seed: int = 0) -> dict:
    keys = jax.random.split(jax.random.key(seed), 7)
    return {
        "hidden_in": draw_hidden_in(jax.random.fold_in(keys[6], 71), 0),
        "norm_gain": jnp.clip(1.0 + 0.18 * jax.random.normal(keys[1], (LAYERS, D), jnp.float32), 0.099609375, 1.8984375).astype(jnp.bfloat16),
        "router_weight": draw_router_weight(jax.random.fold_in(keys[6], 71), 0),
        "expert_scale": jnp.clip(jnp.exp(math.log(16.0) - 2.7725887 * jax.random.uniform(keys[3], (LAYERS, E, D), jnp.float32) ** level_of(keys[3], (LAYERS, E, D), ((0, 4),), -0.2, 0.2)), 1.0, 16.0).astype(jnp.bfloat16),
        "mix_weight": bell_draw(keys[4], (LAYERS, D, D), D ** -0.5, 0.125, ((0, 4),)),
        "routes": draw_routes(jax.random.fold_in(keys[6], 71), 0),
    }


def router_layer(hidden_rows, gain_row, w_router, scale_table, w_mix, chosen_ids):
    state_wide = hidden_rows.astype(jnp.float32)
    mean_square = lax.optimization_barrier(jnp.mean(state_wide * state_wide, axis=-1, keepdims=True))
    normed = state_wide * lax.rsqrt(mean_square + 1e-06) * gain_row.astype(jnp.float32)
    logits = jnp.dot(normed.astype(jnp.bfloat16), w_router, preferred_element_type=jnp.float32)
    exponent = jnp.exp(logits)
    probabilities = exponent / lax.optimization_barrier(jnp.sum(exponent, axis=-1, keepdims=True))
    expert_ids = jnp.arange(w_router.shape[1], dtype=jnp.int32)
    onehot = lax.optimization_barrier(jnp.sum((chosen_ids[:, :, None] == expert_ids[None, None, :]).astype(jnp.float32), axis=1))
    gate_values = (probabilities * onehot).astype(jnp.bfloat16)
    channel_scale = jnp.dot(gate_values, scale_table, preferred_element_type=jnp.float32)
    mixed_rows = (normed * channel_scale).astype(jnp.bfloat16)
    update = jnp.dot(mixed_rows, w_mix, preferred_element_type=jnp.float32)
    updated = (state_wide + update).astype(jnp.bfloat16)
    return (updated, lax.optimization_barrier(jnp.sum(onehot, axis=0)), lax.optimization_barrier(jnp.sum(probabilities, axis=0)))

def reference(hidden_in, norm_gain, router_weight, expert_scale, mix_weight, routes):
    row_total = M * TOK_MB
    hidden_rows = hidden_in.reshape(row_total, D)
    losses = []
    for layer_index in range(LAYERS):
        chosen_ids = routes[layer_index].reshape(row_total, K)
        hidden_rows, counts, prob_sums = router_layer(hidden_rows, norm_gain[layer_index], router_weight[layer_index], expert_scale[layer_index], mix_weight[layer_index], chosen_ids)
        fractions = counts / jnp.float32(row_total * K)
        mean_probs = prob_sums / jnp.float32(row_total)
        losses.append(jnp.float32(E) * jnp.sum(fractions * mean_probs))
    return (hidden_rows.reshape(M, TOK_MB, D), jnp.stack(losses).astype(jnp.float32))
```

```python
import functools

import jax
import jax.numpy as jnp
from jax import lax
from jax.experimental import pallas as pl
from jax.experimental.pallas import tpu as pltpu
from jax.sharding import PartitionSpec as P

MESH = pl.DeviceIdType.MESH


def relay(
    sections,
    shards,
    chunk,
    hidden,
    gain,
    router,
    scale,
    mix,
    routes,
    out,
    loss,
    arrived,
    left,
    weights,
    router_v,
    scale_v,
    gain_v,
    routes_v,
    normed_v,
    normed_b,
    mixed_v,
    stats,
    all_stats,
    in_sem,
    send_sem,
    out_sem,
    weight_sem,
    table_sem,
    stat_send,
    stat_recv,
):
    section = lax.axis_index("section")
    shard = lax.axis_index("dp")
    batches, rows, width = arrived.shape
    experts = router_v.shape[1]
    owned = batches // sections
    pieces = width // chunk
    last = sections - 1

    tables = (
        pltpu.make_async_copy(gain, gain_v, table_sem.at[0]),
        pltpu.make_async_copy(router.at[0], router_v, table_sem.at[1]),
        pltpu.make_async_copy(routes.at[0], routes_v, table_sem.at[2]),
        pltpu.make_async_copy(scale.at[0], scale_v, table_sem.at[3]),
    )

    def own_input(batch):
        return pltpu.make_async_copy(hidden.at[batch], arrived.at[batch], in_sem.at[batch])

    def weight_piece(piece):
        columns = pl.ds(piece * chunk, chunk)
        return pltpu.make_async_copy(
            mix.at[0, :, columns], weights.at[:, columns], weight_sem.at[piece]
        )

    @pl.when(section == 0)
    def _():
        own_input(0).start()

    for table in tables:
        table.start()
    for piece in range(pieces):
        weight_piece(piece).start()

    @pl.when(section == 0)
    def _():
        for batch in range(1, batches):
            own_input(batch).start()

    barrier = pltpu.get_barrier_semaphore()
    for step in range(1, sections):
        pl.semaphore_signal(
            barrier,
            inc=1,
            device_id={"section": lax.rem(section + step, sections)},
            device_id_type=MESH,
        )
    for step in range(1, shards):
        pl.semaphore_signal(
            barrier, inc=1, device_id={"dp": lax.rem(shard + step, shards)}, device_id_type=MESH
        )
    stats[...] = jnp.zeros_like(stats)
    for table in tables:
        table.wait()
    pl.semaphore_wait(barrier, sections - 1 + shards - 1)

    def peer_stats(step):
        return pltpu.make_async_remote_copy(
            src_ref=all_stats.at[shard],
            dst_ref=all_stats.at[shard],
            send_sem=stat_send,
            recv_sem=stat_recv,
            device_id={"dp": lax.rem(shard + step, shards)},
            device_id_type=MESH,
        )

    def one_batch(batch, carry):
        own_input(batch).wait()
        square = jnp.zeros((rows, 128), jnp.float32)
        for at in range(0, width, 128):
            part = arrived[batch, :, at : at + 128].astype(jnp.float32)
            square = square + part * part
        mean_square = jnp.sum(square, axis=-1, keepdims=True) / jnp.float32(width)
        inverse = lax.rsqrt(mean_square + 1e-06)
        for at in range(0, width, 256):
            part = arrived[batch, :, at : at + 256].astype(jnp.float32)
            normed = part * inverse * gain_v[:, at : at + 256].astype(jnp.float32)
            normed_v[:, at : at + 256] = normed
            normed_b[:, at : at + 256] = normed.astype(jnp.bfloat16)
        logits = jnp.dot(normed_b[...], router_v[...], preferred_element_type=jnp.float32)
        exponent = jnp.exp(logits)
        probabilities = exponent / jnp.sum(exponent, axis=-1, keepdims=True)
        ids = routes_v[batch]
        lanes = lax.broadcasted_iota(jnp.int32, (rows, experts), 1)
        onehot = jnp.zeros((rows, experts), jnp.float32)
        for pick in range(ids.shape[1]):
            onehot = onehot + (ids[:, pick : pick + 1] == lanes).astype(jnp.float32)
        gates = (probabilities * onehot).astype(jnp.bfloat16)
        stats[0:1, 0:experts] += jnp.sum(onehot, axis=0, keepdims=True)
        stats[1:2, 0:experts] += jnp.sum(probabilities, axis=0, keepdims=True)

        for at in range(0, width, 256):
            channel = jnp.dot(
                gates, scale_v[:, at : at + 256], preferred_element_type=jnp.float32
            )
            mixed_v[:, at : at + 256] = (normed_v[:, at : at + 256] * channel).astype(jnp.bfloat16)

        @pl.when(batch == batches - 1)
        def _():
            all_stats[shard] = stats[...]

        @pl.when(batch == 0)
        def _():
            for piece in range(pieces):
                weight_piece(piece).wait()

        @pl.when(batch == batches - 1)
        def _():
            for step in range(1, shards):
                peer_stats(step).start()

        owner = batch // owned
        for piece in range(pieces):
            at = piece * chunk
            update = jnp.dot(
                mixed_v[...], weights[:, at : at + chunk], preferred_element_type=jnp.float32
            )
            state = arrived[batch, :, at : at + chunk].astype(jnp.float32)
            left[batch, :, at : at + chunk] = (state + update).astype(jnp.bfloat16)

            @pl.when(section < last)
            def _():
                pltpu.make_async_remote_copy(
                    src_ref=left.at[batch, :, pl.ds(at, chunk)],
                    dst_ref=arrived.at[batch, :, pl.ds(at, chunk)],
                    send_sem=send_sem.at[batch],
                    recv_sem=in_sem.at[batch],
                    device_id={"section": section + 1},
                    device_id_type=MESH,
                ).start()

            @pl.when((section == last) & (owner != last))
            def _():
                pltpu.make_async_remote_copy(
                    src_ref=left.at[batch, :, pl.ds(at, chunk)],
                    dst_ref=out.at[lax.rem(batch, owned), :, pl.ds(at, chunk)],
                    send_sem=send_sem.at[batch],
                    recv_sem=out_sem.at[lax.rem(batch, owned)],
                    device_id={"section": owner},
                    device_id_type=MESH,
                ).start()

            @pl.when((section == last) & (owner == last))
            def _():
                pltpu.make_async_copy(
                    left.at[batch, :, pl.ds(at, chunk)],
                    out.at[lax.rem(batch, owned), :, pl.ds(at, chunk)],
                    out_sem.at[lax.rem(batch, owned)],
                ).start()

        return carry

    lax.fori_loop(0, batches, one_batch, 0)

    for slot in range(owned):
        pltpu.make_async_copy(out.at[slot], out.at[slot], out_sem.at[slot]).wait()
    for batch in range(batches):

        @pl.when((section < last) | (batch // owned != last))
        def _():
            pltpu.make_async_copy(left.at[batch], left.at[batch], send_sem.at[batch]).wait()

    others = all_stats.at[pl.ds(0, shards - 1)]
    pltpu.make_async_copy(others, others, stat_send).wait()
    pltpu.make_async_copy(others, others, stat_recv).wait()
    total = all_stats[0]
    for at in range(1, shards):
        total = total + all_stats[at]
    tokens = jnp.float32(batches * rows * shards)
    fractions = total[0:1, :] / (tokens * jnp.float32(routes_v.shape[2]))
    mean_probs = total[1:2, :] / tokens
    loss[0] = jnp.float32(experts) * jnp.sum(fractions * mean_probs)


def per_device(hidden_in, norm_gain, router_weight, expert_scale, mix_weight, routes):
    sections = lax.axis_size("section")
    shards = lax.axis_size("dp")
    batches, rows, width = hidden_in.shape
    experts = router_weight.shape[2]
    picks = routes.shape[3]
    chunk = 256
    pieces = width // chunk
    anywhere = pl.BlockSpec(memory_space=pl.ANY)
    return pl.pallas_call(
        functools.partial(relay, sections, shards, chunk),
        out_shape=(
            jax.ShapeDtypeStruct((batches // sections, rows, width), jnp.bfloat16),
            jax.ShapeDtypeStruct((1,), jnp.float32),
        ),
        in_specs=[anywhere] * 6,
        out_specs=(anywhere, pl.BlockSpec(memory_space=pltpu.SMEM)),
        scratch_shapes=[
            pltpu.VMEM((batches, rows, width), jnp.bfloat16),
            pltpu.VMEM((batches, rows, width), jnp.bfloat16),
            pltpu.VMEM((width, width), jnp.bfloat16),
            pltpu.VMEM((width, experts), jnp.bfloat16),
            pltpu.VMEM((experts, width), jnp.bfloat16),
            pltpu.VMEM((1, width), jnp.bfloat16),
            pltpu.VMEM((batches, rows, picks), jnp.int32),
            pltpu.VMEM((rows, width), jnp.float32),
            pltpu.VMEM((rows, width), jnp.bfloat16),
            pltpu.VMEM((rows, width), jnp.bfloat16),
            pltpu.VMEM((8, 128), jnp.float32),
            pltpu.VMEM((shards, 8, 128), jnp.float32),
            pltpu.SemaphoreType.DMA((batches,)),
            pltpu.SemaphoreType.DMA((batches,)),
            pltpu.SemaphoreType.DMA((batches // sections,)),
            pltpu.SemaphoreType.DMA((pieces,)),
            pltpu.SemaphoreType.DMA((4,)),
            pltpu.SemaphoreType.DMA,
            pltpu.SemaphoreType.DMA,
        ],
        compiler_params=pltpu.CompilerParams(collective_id=0, has_side_effects=True),
    )(hidden_in, norm_gain, router_weight, expert_scale, mix_weight, routes)


def solution(mesh):
    placed = (
        P(None, "dp", None),
        P("section", None),
        P("section", None, None),
        P("section", None, None),
        P("section", None, None),
        P("section", None, "dp", None),
    )
    return jax.shard_map(
        per_device,
        mesh=mesh,
        in_specs=placed,
        out_specs=(P("section", "dp", None), P("section")),
        check_vma=False,
    )
```

```python
import functools

import jax
import jax.numpy as jnp
from jax import lax
from jax.experimental import pallas as pl
from jax.experimental.pallas import tpu as pltpu
from jax.sharding import PartitionSpec as P

MESH = pl.DeviceIdType.MESH


def relay(
    sections,
    shards,
    chunk,
    group,
    hidden,
    gain,
    router,
    scale,
    mix,
    routes,
    out,
    loss,
    arrived,
    left,
    weights,
    router_v,
    scale_v,
    gain_v,
    routes_v,
    normed_v,
    normed_b,
    mixed_v,
    stats,
    all_stats,
    in_sem,
    send_sem,
    out_sem,
    weight_sem,
    table_sem,
    stat_send,
    stat_recv,
):
    section = lax.axis_index("section")
    shard = lax.axis_index("dp")
    batches, rows, width = hidden.shape
    experts, picks = router_v.shape[0], routes_v.shape[1]
    groups, tall = batches // group, group * rows
    owned = batches // sections
    pieces = width // chunk
    last = sections - 1

    tables = (
        pltpu.make_async_copy(gain, gain_v, table_sem.at[0]),
        pltpu.make_async_copy(router, router_v, table_sem.at[1]),
        pltpu.make_async_copy(routes.at[0], routes_v, table_sem.at[2]),
        pltpu.make_async_copy(scale.at[0], scale_v, table_sem.at[3]),
    )

    def own_input(batch):
        place = arrived.at[batch // group, pl.ds(batch % group * rows, rows), :]
        return pltpu.make_async_copy(hidden.at[batch], place, in_sem.at[batch // group])

    def weight_piece(piece):
        columns = pl.ds(piece * chunk, chunk)
        return pltpu.make_async_copy(
            mix.at[0, :, columns], weights.at[:, columns], weight_sem.at[piece]
        )

    @pl.when(section == 0)
    def _():
        for batch in range(group):
            own_input(batch).start()

    for table in tables:
        table.start()
    for piece in range(pieces):
        weight_piece(piece).start()

    @pl.when(section == 0)
    def _():
        for batch in range(group, batches):
            own_input(batch).start()

    barrier = pltpu.get_barrier_semaphore()
    for step in range(1, sections):
        pl.semaphore_signal(
            barrier,
            inc=1,
            device_id={"section": lax.rem(section + step, sections)},
            device_id_type=MESH,
        )
    for step in range(1, shards):
        pl.semaphore_signal(
            barrier, inc=1, device_id={"dp": lax.rem(shard + step, shards)}, device_id_type=MESH
        )
    stats[...] = jnp.zeros_like(stats)
    for table in tables:
        table.wait()

    def peer_stats(step):
        return pltpu.make_async_remote_copy(
            src_ref=all_stats.at[shard],
            dst_ref=all_stats.at[shard],
            send_sem=stat_send,
            recv_sem=stat_recv,
            device_id={"dp": lax.rem(shard + step, shards)},
            device_id_type=MESH,
        )

    def one_group(at_group, carry):
        ids = jnp.concatenate([routes_v[at_group * group + k] for k in range(group)], axis=1)
        sublanes = lax.broadcasted_iota(jnp.int32, (128, tall), 0)
        standing = jnp.zeros((128, tall), jnp.float32)
        for pick in range(picks):
            standing = standing + (ids[pick : pick + 1, :] == sublanes).astype(jnp.float32)
        onehot = jnp.transpose(standing)[:, 0:experts]
        pltpu.make_async_copy(
            arrived.at[at_group], arrived.at[at_group], in_sem.at[at_group]
        ).wait()
        square = jnp.zeros((tall, 128), jnp.float32)
        for at in range(0, width, 128):
            part = arrived[at_group, :, at : at + 128].astype(jnp.float32)
            square = square + part * part
        mean_square = jnp.sum(square, axis=-1, keepdims=True) / jnp.float32(width)
        inverse = lax.rsqrt(mean_square + 1e-06)
        for at in range(0, width, 256):
            part = arrived[at_group, :, at : at + 256].astype(jnp.float32)
            normed = part * inverse * gain_v[:, at : at + 256].astype(jnp.float32)
            normed_v[:, at : at + 256] = normed
            normed_b[:, at : at + 256] = normed.astype(jnp.bfloat16)
        logits = lax.dot_general(
            normed_b[...],
            router_v[...],
            (((1,), (1,)), ((), ())),
            preferred_element_type=jnp.float32,
        )
        exponent = jnp.exp(logits)
        probabilities = exponent / jnp.sum(exponent, axis=-1, keepdims=True)
        gates = (probabilities * onehot).astype(jnp.bfloat16)
        stats[0:1, 0:experts] += jnp.sum(onehot, axis=0, keepdims=True)
        stats[1:2, 0:experts] += jnp.sum(probabilities, axis=0, keepdims=True)

        for at in range(0, width, 256):
            channel = jnp.dot(
                gates, scale_v[:, at : at + 256], preferred_element_type=jnp.float32
            )
            mixed_v[:, at : at + 256] = (normed_v[:, at : at + 256] * channel).astype(jnp.bfloat16)

        @pl.when(at_group == groups - 1)
        def _():
            all_stats[shard] = stats[...]

        @pl.when(at_group == 0)
        def _():
            pl.semaphore_wait(barrier, sections - 1 + shards - 1)

        @pl.when(at_group == groups - 1)
        def _():
            for step in range(1, shards):
                peer_stats(step).start()

        for piece in range(pieces):
            at = piece * chunk
            columns = pl.ds(at, chunk)

            @pl.when(at_group == 0)
            def _():
                weight_piece(piece).wait()

            update = jnp.dot(
                mixed_v[...], weights[:, at : at + chunk], preferred_element_type=jnp.float32
            )
            state = arrived[at_group, :, at : at + chunk].astype(jnp.float32)
            left[at_group, :, at : at + chunk] = (state + update).astype(jnp.bfloat16)

            @pl.when(section < last)
            def _():
                pltpu.make_async_remote_copy(
                    src_ref=left.at[at_group, :, columns],
                    dst_ref=arrived.at[at_group, :, columns],
                    send_sem=send_sem.at[at_group],
                    recv_sem=in_sem.at[at_group],
                    device_id={"section": section + 1},
                    device_id_type=MESH,
                ).start()

            for k in range(group):
                batch = at_group * group + k
                owner = batch // owned

                @pl.when((section == last) & (owner != last))
                def _():
                    pltpu.make_async_remote_copy(
                        src_ref=left.at[at_group, pl.ds(k * rows, rows), columns],
                        dst_ref=out.at[lax.rem(batch, owned), :, columns],
                        send_sem=send_sem.at[at_group],
                        recv_sem=out_sem.at[lax.rem(batch, owned)],
                        device_id={"section": owner},
                        device_id_type=MESH,
                    ).start()

        return carry

    lax.fori_loop(0, groups, one_group, 0)

    @pl.when(section == last)
    def _():
        for slot in range(owned):
            batch = batches - owned + slot
            out[slot] = left[batch // group, pl.ds(batch % group * rows, rows), :]

    @pl.when(section != last)
    def _():
        for slot in range(owned):
            pltpu.make_async_copy(out.at[slot], out.at[slot], out_sem.at[slot]).wait()

    for batch in range(batches):
        sent = left.at[batch // group, pl.ds(batch % group * rows, rows), :]

        @pl.when((section < last) | (batch // owned != last))
        def _():
            pltpu.make_async_copy(sent, sent, send_sem.at[batch // group]).wait()

    others = all_stats.at[pl.ds(0, shards - 1)]
    pltpu.make_async_copy(others, others, stat_send).wait()
    pltpu.make_async_copy(others, others, stat_recv).wait()
    total = all_stats[0]
    for at in range(1, shards):
        total = total + all_stats[at]
    tokens = jnp.float32(batches * rows * shards)
    fractions = total[0:1, :] / (tokens * jnp.float32(picks))
    mean_probs = total[1:2, :] / tokens
    loss[0] = jnp.float32(experts) * jnp.sum(fractions * mean_probs)


def per_device(hidden_in, norm_gain, router_weight, expert_scale, mix_weight, routes):
    sections = lax.axis_size("section")
    shards = lax.axis_size("dp")
    batches, rows, width = hidden_in.shape
    experts = router_weight.shape[2]
    picks = routes.shape[3]
    group = 2 if batches % 2 == 0 else 1
    groups, tall = batches // group, group * rows
    chunk = 256
    pieces = width // chunk
    anywhere = pl.BlockSpec(memory_space=pl.ANY)
    return pl.pallas_call(
        functools.partial(relay, sections, shards, chunk, group),
        out_shape=(
            jax.ShapeDtypeStruct((batches // sections, rows, width), jnp.bfloat16),
            jax.ShapeDtypeStruct((1,), jnp.float32),
        ),
        in_specs=[anywhere] * 6,
        out_specs=(pl.BlockSpec(memory_space=pltpu.VMEM), pl.BlockSpec(memory_space=pltpu.SMEM)),
        scratch_shapes=[
            pltpu.VMEM((groups, tall, width), jnp.bfloat16),
            pltpu.VMEM((groups, tall, width), jnp.bfloat16),
            pltpu.VMEM((width, width), jnp.bfloat16),
            pltpu.VMEM((experts, width), jnp.bfloat16),
            pltpu.VMEM((experts, width), jnp.bfloat16),
            pltpu.VMEM((1, width), jnp.bfloat16),
            pltpu.VMEM((batches, picks, rows), jnp.int32),
            pltpu.VMEM((tall, width), jnp.float32),
            pltpu.VMEM((tall, width), jnp.bfloat16),
            pltpu.VMEM((tall, width), jnp.bfloat16),
            pltpu.VMEM((8, 128), jnp.float32),
            pltpu.VMEM((shards, 8, 128), jnp.float32),
            pltpu.SemaphoreType.DMA((groups,)),
            pltpu.SemaphoreType.DMA((groups,)),
            pltpu.SemaphoreType.DMA((batches // sections,)),
            pltpu.SemaphoreType.DMA((pieces,)),
            pltpu.SemaphoreType.DMA((4,)),
            pltpu.SemaphoreType.DMA,
            pltpu.SemaphoreType.DMA,
        ],
        compiler_params=pltpu.CompilerParams(collective_id=0, has_side_effects=True),
    )(
        hidden_in,
        norm_gain,
        jnp.transpose(router_weight[0]),
        expert_scale,
        mix_weight,
        jnp.swapaxes(routes, 2, 3),
    )


def solution(mesh):
    placed = (
        P(None, "dp", None),
        P("section", None),
        P("section", None, None),
        P("section", None, None),
        P("section", None, None),
        P("section", None, "dp", None),
    )
    return jax.shard_map(
        per_device,
        mesh=mesh,
        in_specs=placed,
        out_specs=(P("section", "dp", None), P("section")),
        check_vma=False,
    )
```

```python
import functools

import jax
import jax.numpy as jnp
from jax import lax
from jax.experimental import pallas as pl
from jax.experimental.pallas import tpu as pltpu
from jax.sharding import PartitionSpec as P

MESH = pl.DeviceIdType.MESH


def relay(
    sections,
    shards,
    chunk,
    group,
    hidden,
    gain,
    router,
    scale,
    mix,
    routes,
    out,
    loss,
    arrived,
    left,
    weights,
    router_v,
    scale_v,
    gain_v,
    routes_v,
    normed_b,
    mixed_v,
    stats,
    all_stats,
    in_sem,
    send_sem,
    out_sem,
    weight_sem,
    table_sem,
    stat_send,
    stat_recv,
):
    section = lax.axis_index("section")
    shard = lax.axis_index("dp")
    batches, rows, width = hidden.shape
    experts, picks = router_v.shape[0], routes_v.shape[1]
    groups, tall = batches // group, group * rows
    owned = batches // sections
    pieces = width // chunk
    last = sections - 1

    tables = (
        pltpu.make_async_copy(gain, gain_v, table_sem.at[0]),
        pltpu.make_async_copy(router, router_v, table_sem.at[1]),
        pltpu.make_async_copy(routes.at[0], routes_v, table_sem.at[2]),
        pltpu.make_async_copy(scale.at[0], scale_v, table_sem.at[3]),
    )

    def own_input(batch):
        place = arrived.at[batch // group, pl.ds(batch % group * rows, rows), :]
        return pltpu.make_async_copy(hidden.at[batch], place, in_sem.at[batch // group])

    def weight_piece(piece):
        columns = pl.ds(piece * chunk, chunk)
        return pltpu.make_async_copy(
            mix.at[0, :, columns], weights.at[:, columns], weight_sem.at[piece]
        )

    @pl.when(section == 0)
    def _():
        for batch in range(group):
            own_input(batch).start()

    for table in tables:
        table.start()
    for piece in range(pieces):
        weight_piece(piece).start()

    @pl.when(section == 0)
    def _():
        for batch in range(group, batches):
            own_input(batch).start()

    barrier = pltpu.get_barrier_semaphore()
    for step in range(1, sections):
        pl.semaphore_signal(
            barrier,
            inc=1,
            device_id={"section": lax.rem(section + step, sections)},
            device_id_type=MESH,
        )
    for step in range(1, shards):
        pl.semaphore_signal(
            barrier, inc=1, device_id={"dp": lax.rem(shard + step, shards)}, device_id_type=MESH
        )
    stats[...] = jnp.zeros_like(stats)
    for table in tables:
        table.wait()

    def peer_stats(step):
        return pltpu.make_async_remote_copy(
            src_ref=all_stats.at[shard],
            dst_ref=all_stats.at[shard],
            send_sem=stat_send,
            recv_sem=stat_recv,
            device_id={"dp": lax.rem(shard + step, shards)},
            device_id_type=MESH,
        )

    def one_group(at_group, carry):
        ids = jnp.concatenate([routes_v[at_group * group + k] for k in range(group)], axis=1)
        sublanes = lax.broadcasted_iota(jnp.int32, (128, tall), 0)
        standing = jnp.zeros((128, tall), jnp.float32)
        for pick in range(picks):
            standing = standing + (ids[pick : pick + 1, :] == sublanes).astype(jnp.float32)
        onehot = jnp.transpose(standing)[:, 0:experts]
        pltpu.make_async_copy(
            arrived.at[at_group], arrived.at[at_group], in_sem.at[at_group]
        ).wait()
        square = jnp.zeros((tall, 128), jnp.float32)
        for at in range(0, width, 128):
            part = arrived[at_group, :, at : at + 128].astype(jnp.float32)
            square = square + part * part
        mean_square = jnp.sum(square, axis=-1, keepdims=True) / jnp.float32(width)
        inverse = lax.rsqrt(mean_square + 1e-06)
        for at in range(0, width, 256):
            part = arrived[at_group, :, at : at + 256].astype(jnp.float32)
            normed = part * inverse * gain_v[:, at : at + 256].astype(jnp.float32)
            normed_b[:, at : at + 256] = normed.astype(jnp.bfloat16)
        logits = lax.dot_general(
            normed_b[...],
            router_v[...],
            (((1,), (1,)), ((), ())),
            preferred_element_type=jnp.float32,
        )
        exponent = jnp.exp(logits)
        probabilities = exponent / jnp.sum(exponent, axis=-1, keepdims=True)
        gates = (probabilities * onehot).astype(jnp.bfloat16)
        stats[0:1, 0:experts] += jnp.sum(onehot, axis=0, keepdims=True)
        stats[1:2, 0:experts] += jnp.sum(probabilities, axis=0, keepdims=True)

        for at in range(0, width, chunk):
            channel = jnp.dot(
                gates, scale_v[:, at : at + chunk], preferred_element_type=jnp.float32
            )
            part = arrived[at_group, :, at : at + chunk].astype(jnp.float32)
            normed = part * inverse * gain_v[:, at : at + chunk].astype(jnp.float32)
            mixed_v[:, at : at + chunk] = (normed * channel).astype(jnp.bfloat16)

        @pl.when(at_group == groups - 1)
        def _():
            all_stats[shard] = stats[...]

        @pl.when(at_group == 0)
        def _():
            pl.semaphore_wait(barrier, sections - 1 + shards - 1)

        @pl.when(at_group == groups - 1)
        def _():
            for step in range(1, shards):
                peer_stats(step).start()

        for piece in range(pieces):
            at = piece * chunk
            columns = pl.ds(at, chunk)

            @pl.when(at_group == 0)
            def _():
                weight_piece(piece).wait()

            update = jnp.dot(
                mixed_v[...], weights[:, at : at + chunk], preferred_element_type=jnp.float32
            )
            state = arrived[at_group, :, at : at + chunk].astype(jnp.float32)
            left[at_group, :, at : at + chunk] = (state + update).astype(jnp.bfloat16)

            @pl.when(section < last)
            def _():
                pltpu.make_async_remote_copy(
                    src_ref=left.at[at_group, :, columns],
                    dst_ref=arrived.at[at_group, :, columns],
                    send_sem=send_sem.at[at_group],
                    recv_sem=in_sem.at[at_group],
                    device_id={"section": section + 1},
                    device_id_type=MESH,
                ).start()

            for k in range(group):
                batch = at_group * group + k
                owner = batch // owned

                @pl.when((section == last) & (owner != last))
                def _():
                    pltpu.make_async_remote_copy(
                        src_ref=left.at[at_group, pl.ds(k * rows, rows), columns],
                        dst_ref=out.at[lax.rem(batch, owned), :, columns],
                        send_sem=send_sem.at[at_group],
                        recv_sem=out_sem.at[lax.rem(batch, owned)],
                        device_id={"section": owner},
                        device_id_type=MESH,
                    ).start()

        return carry

    lax.fori_loop(0, groups, one_group, 0)

    @pl.when(section == last)
    def _():
        for slot in range(owned):
            batch = batches - owned + slot
            out[slot] = left[batch // group, pl.ds(batch % group * rows, rows), :]

    @pl.when(section != last)
    def _():
        for slot in range(owned):
            pltpu.make_async_copy(out.at[slot], out.at[slot], out_sem.at[slot]).wait()

    for batch in range(batches):
        sent = left.at[batch // group, pl.ds(batch % group * rows, rows), :]

        @pl.when((section < last) | (batch // owned != last))
        def _():
            pltpu.make_async_copy(sent, sent, send_sem.at[batch // group]).wait()

    others = all_stats.at[pl.ds(0, shards - 1)]
    pltpu.make_async_copy(others, others, stat_send).wait()
    pltpu.make_async_copy(others, others, stat_recv).wait()
    total = all_stats[0]
    for at in range(1, shards):
        total = total + all_stats[at]
    tokens = jnp.float32(batches * rows * shards)
    fractions = total[0:1, :] / (tokens * jnp.float32(picks))
    mean_probs = total[1:2, :] / tokens
    loss[0] = jnp.float32(experts) * jnp.sum(fractions * mean_probs)


def per_device(hidden_in, norm_gain, router_weight, expert_scale, mix_weight, routes):
    sections = lax.axis_size("section")
    shards = lax.axis_size("dp")
    batches, rows, width = hidden_in.shape
    experts = router_weight.shape[2]
    picks = routes.shape[3]
    group = 2 if batches % 2 == 0 else 1
    groups, tall = batches // group, group * rows
    chunk = 512
    pieces = width // chunk
    anywhere = pl.BlockSpec(memory_space=pl.ANY)
    return pl.pallas_call(
        functools.partial(relay, sections, shards, chunk, group),
        out_shape=(
            jax.ShapeDtypeStruct((batches // sections, rows, width), jnp.bfloat16),
            jax.ShapeDtypeStruct((1,), jnp.float32),
        ),
        in_specs=[anywhere] * 6,
        out_specs=(pl.BlockSpec(memory_space=pltpu.VMEM), pl.BlockSpec(memory_space=pltpu.SMEM)),
        scratch_shapes=[
            pltpu.VMEM((groups, tall, width), jnp.bfloat16),
            pltpu.VMEM((groups, tall, width), jnp.bfloat16),
            pltpu.VMEM((width, width), jnp.bfloat16),
            pltpu.VMEM((experts, width), jnp.bfloat16),
            pltpu.VMEM((experts, width), jnp.bfloat16),
            pltpu.VMEM((1, width), jnp.bfloat16),
            pltpu.VMEM((batches, picks, rows), jnp.int32),
            pltpu.VMEM((tall, width), jnp.bfloat16),
            pltpu.VMEM((tall, width), jnp.bfloat16),
            pltpu.VMEM((8, 128), jnp.float32),
            pltpu.VMEM((shards, 8, 128), jnp.float32),
            pltpu.SemaphoreType.DMA((groups,)),
            pltpu.SemaphoreType.DMA((groups,)),
            pltpu.SemaphoreType.DMA((batches // sections,)),
            pltpu.SemaphoreType.DMA((pieces,)),
            pltpu.SemaphoreType.DMA((4,)),
            pltpu.SemaphoreType.DMA,
            pltpu.SemaphoreType.DMA,
        ],
        compiler_params=pltpu.CompilerParams(collective_id=0, has_side_effects=True),
    )(
        hidden_in,
        norm_gain,
        jnp.transpose(router_weight[0]),
        expert_scale,
        mix_weight,
        jnp.swapaxes(routes, 2, 3),
    )


def solution(mesh):
    placed = (
        P(None, "dp", None),
        P("section", None),
        P("section", None, None),
        P("section", None, None),
        P("section", None, None),
        P("section", None, "dp", None),
    )
    return jax.shard_map(
        per_device,
        mesh=mesh,
        in_specs=placed,
        out_specs=(P("section", "dp", None), P("section")),
        check_vma=False,
    )
```

```python
import functools

import jax
import jax.numpy as jnp
from jax import lax
from jax.experimental import pallas as pl
from jax.experimental.pallas import tpu as pltpu
from jax.sharding import PartitionSpec as P

MESH = pl.DeviceIdType.MESH


def relay(
    sections,
    shards,
    chunk,
    group,
    hidden,
    gain,
    router,
    scale,
    mix,
    routes,
    out,
    loss,
    arrived,
    left,
    weights,
    router_v,
    scale_v,
    gain_v,
    routes_v,
    normed_b,
    mixed_v,
    stats,
    all_stats,
    in_sem,
    send_sem,
    out_sem,
    weight_sem,
    table_sem,
    stat_send,
    stat_recv,
):
    section = lax.axis_index("section")
    shard = lax.axis_index("dp")
    batches, rows, width = hidden.shape
    experts, picks = router_v.shape[0], routes_v.shape[1]
    groups, tall = batches // group, group * rows
    owned = batches // sections
    pieces = width // chunk
    last = sections - 1

    tables = (
        pltpu.make_async_copy(gain, gain_v, table_sem.at[0]),
        pltpu.make_async_copy(router, router_v, table_sem.at[1]),
        pltpu.make_async_copy(routes.at[0], routes_v, table_sem.at[2]),
        pltpu.make_async_copy(scale.at[0], scale_v, table_sem.at[3]),
    )

    def own_input(batch):
        place = arrived.at[batch // group, pl.ds(batch % group * rows, rows), :]
        return pltpu.make_async_copy(hidden.at[batch], place, in_sem.at[batch // group])

    def weight_piece(piece):
        columns = pl.ds(piece * chunk, chunk)
        return pltpu.make_async_copy(
            mix.at[0, :, columns], weights.at[:, columns], weight_sem.at[piece]
        )

    @pl.when(section == 0)
    def _():
        for batch in range(group):
            own_input(batch).start()

    for table in tables:
        table.start()
    for piece in range(pieces):
        weight_piece(piece).start()

    @pl.when(section == 0)
    def _():
        for batch in range(group, batches):
            own_input(batch).start()

    barrier = pltpu.get_barrier_semaphore()
    for step in range(1, sections):
        pl.semaphore_signal(
            barrier,
            inc=1,
            device_id={"section": lax.rem(section + step, sections)},
            device_id_type=MESH,
        )
    for step in range(1, shards):
        pl.semaphore_signal(
            barrier, inc=1, device_id={"dp": lax.rem(shard + step, shards)}, device_id_type=MESH
        )
    stats[...] = jnp.zeros_like(stats)
    for table in tables:
        table.wait()

    def peer_stats(step):
        return pltpu.make_async_remote_copy(
            src_ref=all_stats.at[shard],
            dst_ref=all_stats.at[shard],
            send_sem=stat_send,
            recv_sem=stat_recv,
            device_id={"dp": lax.rem(shard + step, shards)},
            device_id_type=MESH,
        )

    def one_group(at_group, carry):
        ids = jnp.concatenate([routes_v[at_group * group + k] for k in range(group)], axis=1)
        sublanes = lax.broadcasted_iota(jnp.int32, (128, tall), 0)
        standing = jnp.zeros((128, tall), jnp.float32)
        for pick in range(picks):
            standing = standing + (ids[pick : pick + 1, :] == sublanes).astype(jnp.float32)
        onehot = jnp.transpose(standing)[:, 0:experts]
        pltpu.make_async_copy(
            arrived.at[at_group], arrived.at[at_group], in_sem.at[at_group]
        ).wait()
        square = jnp.zeros((tall, 128), jnp.float32)
        for at in range(0, width, 128):
            part = arrived[at_group, :, at : at + 128].astype(jnp.float32)
            square = square + part * part
        mean_square = jnp.sum(square, axis=-1, keepdims=True) / jnp.float32(width)
        inverse = lax.rsqrt(mean_square + 1e-06)
        for at in range(0, width, 256):
            part = arrived[at_group, :, at : at + 256].astype(jnp.float32)
            normed = part * inverse * gain_v[:, at : at + 256].astype(jnp.float32)
            normed_b[:, at : at + 256] = normed.astype(jnp.bfloat16)
        logits = lax.dot_general(
            normed_b[...],
            router_v[...],
            (((1,), (1,)), ((), ())),
            preferred_element_type=jnp.float32,
        )
        exponent = jnp.exp(logits)
        probabilities = exponent / jnp.sum(exponent, axis=-1, keepdims=True)
        gates = (probabilities * onehot).astype(jnp.bfloat16)
        stats[0:1, 0:experts] += jnp.sum(onehot, axis=0, keepdims=True)
        stats[1:2, 0:experts] += jnp.sum(probabilities, axis=0, keepdims=True)

        for at in range(0, width, chunk):
            channel = jnp.dot(
                gates, scale_v[:, at : at + chunk], preferred_element_type=jnp.float32
            )
            part = arrived[at_group, :, at : at + chunk].astype(jnp.float32)
            normed = part * inverse * gain_v[:, at : at + chunk].astype(jnp.float32)
            mixed_v[:, at : at + chunk] = (normed * channel).astype(jnp.bfloat16)

        @pl.when(at_group == groups - 1)
        def _():
            all_stats[shard] = stats[...]

        @pl.when(at_group == 0)
        def _():
            pl.semaphore_wait(barrier, sections - 1 + shards - 1)

        @pl.when(at_group == groups - 1)
        def _():
            for step in range(1, shards):
                peer_stats(step).start()

        for piece in range(pieces):
            at = piece * chunk
            columns = pl.ds(at, chunk)

            @pl.when(at_group == 0)
            def _():
                weight_piece(piece).wait()

            update = jnp.dot(
                mixed_v[...], weights[:, at : at + chunk], preferred_element_type=jnp.float32
            )
            state = arrived[at_group, :, at : at + chunk].astype(jnp.float32)
            left[at_group, :, at : at + chunk] = (state + update).astype(jnp.bfloat16)

            @pl.when(section < last)
            def _():
                pltpu.make_async_remote_copy(
                    src_ref=left.at[at_group, :, columns],
                    dst_ref=arrived.at[at_group, :, columns],
                    send_sem=send_sem.at[at_group],
                    recv_sem=in_sem.at[at_group],
                    device_id={"section": section + 1},
                    device_id_type=MESH,
                ).start()

            for k in range(group):
                batch = at_group * group + k
                owner = batch // owned

                @pl.when((section == last) & (owner != last))
                def _():
                    pltpu.make_async_remote_copy(
                        src_ref=left.at[at_group, pl.ds(k * rows, rows), columns],
                        dst_ref=out.at[lax.rem(batch, owned), :, columns],
                        send_sem=send_sem.at[at_group],
                        recv_sem=out_sem.at[lax.rem(batch, owned)],
                        device_id={"section": owner},
                        device_id_type=MESH,
                    ).start()

        return carry

    lax.fori_loop(0, groups, one_group, 0)

    @pl.when(section == last)
    def _():
        for slot in range(owned):
            batch = batches - owned + slot
            out[slot] = left[batch // group, pl.ds(batch % group * rows, rows), :]

    @pl.when(section != last)
    def _():
        for slot in range(owned):
            pltpu.make_async_copy(out.at[slot], out.at[slot], out_sem.at[slot]).wait()

    for batch in range(batches):
        sent = left.at[batch // group, pl.ds(batch % group * rows, rows), :]

        @pl.when((section < last) | (batch // owned != last))
        def _():
            pltpu.make_async_copy(sent, sent, send_sem.at[batch // group]).wait()

    others = all_stats.at[pl.ds(0, shards - 1)]
    pltpu.make_async_copy(others, others, stat_send).wait()
    pltpu.make_async_copy(others, others, stat_recv).wait()
    total = all_stats[0]
    for at in range(1, shards):
        total = total + all_stats[at]
    tokens = jnp.float32(batches * rows * shards)
    fractions = total[0:1, :] / (tokens * jnp.float32(picks))
    mean_probs = total[1:2, :] / tokens
    loss[0] = jnp.float32(experts) * jnp.sum(fractions * mean_probs)


def per_device(hidden_in, norm_gain, router_weight, expert_scale, mix_weight, routes):
    sections = lax.axis_size("section")
    shards = lax.axis_size("dp")
    batches, rows, width = hidden_in.shape
    experts = router_weight.shape[2]
    picks = routes.shape[3]
    group = 1
    groups, tall = batches // group, group * rows
    chunk = 512
    pieces = width // chunk
    anywhere = pl.BlockSpec(memory_space=pl.ANY)
    return pl.pallas_call(
        functools.partial(relay, sections, shards, chunk, group),
        out_shape=(
            jax.ShapeDtypeStruct((batches // sections, rows, width), jnp.bfloat16),
            jax.ShapeDtypeStruct((1,), jnp.float32),
        ),
        in_specs=[anywhere] * 6,
        out_specs=(pl.BlockSpec(memory_space=pltpu.VMEM), pl.BlockSpec(memory_space=pltpu.SMEM)),
        scratch_shapes=[
            pltpu.VMEM((groups, tall, width), jnp.bfloat16),
            pltpu.VMEM((groups, tall, width), jnp.bfloat16),
            pltpu.VMEM((width, width), jnp.bfloat16),
            pltpu.VMEM((experts, width), jnp.bfloat16),
            pltpu.VMEM((experts, width), jnp.bfloat16),
            pltpu.VMEM((1, width), jnp.bfloat16),
            pltpu.VMEM((batches, picks, rows), jnp.int32),
            pltpu.VMEM((tall, width), jnp.bfloat16),
            pltpu.VMEM((tall, width), jnp.bfloat16),
            pltpu.VMEM((8, 128), jnp.float32),
            pltpu.VMEM((shards, 8, 128), jnp.float32),
            pltpu.SemaphoreType.DMA((groups,)),
            pltpu.SemaphoreType.DMA((groups,)),
            pltpu.SemaphoreType.DMA((batches // sections,)),
            pltpu.SemaphoreType.DMA((pieces,)),
            pltpu.SemaphoreType.DMA((4,)),
            pltpu.SemaphoreType.DMA,
            pltpu.SemaphoreType.DMA,
        ],
        compiler_params=pltpu.CompilerParams(collective_id=0, has_side_effects=True),
    )(
        hidden_in,
        norm_gain,
        jnp.transpose(router_weight[0]),
        expert_scale,
        mix_weight,
        jnp.swapaxes(routes, 2, 3),
    )


def solution(mesh):
    placed = (
        P(None, "dp", None),
        P("section", None),
        P("section", None, None),
        P("section", None, None),
        P("section", None, None),
        P("section", None, "dp", None),
    )
    return jax.shard_map(
        per_device,
        mesh=mesh,
        in_specs=placed,
        out_specs=(P("section", "dp", None), P("section")),
        check_vma=False,
    )
```

```python
import functools

import jax
import jax.numpy as jnp
from jax import lax
from jax.experimental import pallas as pl
from jax.experimental.pallas import tpu as pltpu
from jax.sharding import PartitionSpec as P

MESH = pl.DeviceIdType.MESH


def relay(
    sections,
    shards,
    chunk,
    group,
    hidden,
    gain,
    router,
    scale,
    mix,
    routes,
    out,
    loss,
    arrived,
    left,
    weights,
    router_v,
    scale_v,
    gain_v,
    routes_v,
    normed_b,
    mixed_v,
    stats,
    all_stats,
    in_sem,
    send_sem,
    out_sem,
    weight_sem,
    table_sem,
    stat_send,
    stat_recv,
):
    section = lax.axis_index("section")
    shard = lax.axis_index("dp")
    batches, rows, width = hidden.shape
    experts, picks = router_v.shape[0], routes_v.shape[1]
    groups, tall = batches // group, group * rows
    owned = batches // sections
    pieces = width // chunk
    last = sections - 1

    tables = (
        pltpu.make_async_copy(gain, gain_v, table_sem.at[0]),
        pltpu.make_async_copy(router, router_v, table_sem.at[1]),
        pltpu.make_async_copy(routes.at[0], routes_v, table_sem.at[2]),
        pltpu.make_async_copy(scale.at[0], scale_v, table_sem.at[3]),
    )

    def own_input(batch):
        place = arrived.at[batch // group, pl.ds(batch % group * rows, rows), :]
        return pltpu.make_async_copy(hidden.at[batch], place, in_sem.at[batch // group])

    def weight_piece(piece):
        columns = pl.ds(piece * chunk, chunk)
        return pltpu.make_async_copy(
            mix.at[0, :, columns], weights.at[:, columns], weight_sem.at[piece]
        )

    @pl.when(section == 0)
    def _():
        for batch in range(group):
            own_input(batch).start()

    for table in tables:
        table.start()
    for piece in range(pieces):
        weight_piece(piece).start()

    @pl.when(section == 0)
    def _():
        for batch in range(group, batches):
            own_input(batch).start()

    barrier = pltpu.get_barrier_semaphore()
    for step in range(1, sections):
        pl.semaphore_signal(
            barrier,
            inc=1,
            device_id={"section": lax.rem(section + step, sections)},
            device_id_type=MESH,
        )
    for step in range(1, shards):
        pl.semaphore_signal(
            barrier, inc=1, device_id={"dp": lax.rem(shard + step, shards)}, device_id_type=MESH
        )
    stats[...] = jnp.zeros_like(stats)
    for table in tables:
        table.wait()

    def peer_stats(step):
        return pltpu.make_async_remote_copy(
            src_ref=all_stats.at[shard],
            dst_ref=all_stats.at[shard],
            send_sem=stat_send,
            recv_sem=stat_recv,
            device_id={"dp": lax.rem(shard + step, shards)},
            device_id_type=MESH,
        )

    def one_group(at_group, carry):
        ids = jnp.concatenate([routes_v[at_group * group + k] for k in range(group)], axis=1)
        sublanes = lax.broadcasted_iota(jnp.int32, (128, tall), 0)
        standing = jnp.zeros((128, tall), jnp.float32)
        for pick in range(picks):
            standing = standing + (ids[pick : pick + 1, :] == sublanes).astype(jnp.float32)
        onehot = jnp.transpose(standing)[:, 0:experts]
        pltpu.make_async_copy(
            arrived.at[at_group], arrived.at[at_group], in_sem.at[at_group]
        ).wait()
        square = jnp.zeros((tall, 128), jnp.float32)
        for at in range(0, width, 128):
            part = arrived[at_group, :, at : at + 128].astype(jnp.float32)
            square = square + part * part
        mean_square = jnp.sum(square, axis=-1, keepdims=True) / jnp.float32(width)
        inverse = lax.rsqrt(mean_square + 1e-06)
        for at in range(0, width, 256):
            part = arrived[at_group, :, at : at + 256].astype(jnp.float32)
            normed = part * inverse * gain_v[:, at : at + 256].astype(jnp.float32)
            normed_b[:, at : at + 256] = normed.astype(jnp.bfloat16)
        logits = lax.dot_general(
            normed_b[...],
            router_v[...],
            (((1,), (1,)), ((), ())),
            preferred_element_type=jnp.float32,
        )
        exponent = jnp.exp(logits)
        probabilities = exponent / jnp.sum(exponent, axis=-1, keepdims=True)
        gates = (probabilities * onehot).astype(jnp.bfloat16)
        stats[0:1, 0:experts] += jnp.sum(onehot, axis=0, keepdims=True)
        stats[1:2, 0:experts] += jnp.sum(probabilities, axis=0, keepdims=True)

        for at in range(0, width, chunk):
            channel = jnp.dot(
                gates, scale_v[:, at : at + chunk], preferred_element_type=jnp.float32
            )
            part = arrived[at_group, :, at : at + chunk].astype(jnp.float32)
            normed = part * inverse * gain_v[:, at : at + chunk].astype(jnp.float32)
            mixed_v[:, at : at + chunk] = (normed * channel).astype(jnp.bfloat16)

        @pl.when(at_group == groups - 1)
        def _():
            all_stats[shard] = stats[...]

        @pl.when(at_group == 0)
        def _():
            pl.semaphore_wait(barrier, sections - 1 + shards - 1)

        @pl.when(at_group == groups - 1)
        def _():
            for step in range(1, shards):
                peer_stats(step).start()

        for piece in range(pieces):
            at = piece * chunk
            columns = pl.ds(at, chunk)

            @pl.when(at_group == 0)
            def _():
                weight_piece(piece).wait()

            update = jnp.dot(
                mixed_v[...], weights[:, at : at + chunk], preferred_element_type=jnp.float32
            )
            state = arrived[at_group, :, at : at + chunk].astype(jnp.float32)
            left[at_group, :, at : at + chunk] = (state + update).astype(jnp.bfloat16)

            @pl.when(section < last)
            def _():
                pltpu.make_async_remote_copy(
                    src_ref=left.at[at_group, :, columns],
                    dst_ref=arrived.at[at_group, :, columns],
                    send_sem=send_sem.at[at_group],
                    recv_sem=in_sem.at[at_group],
                    device_id={"section": section + 1},
                    device_id_type=MESH,
                ).start()

            for k in range(group):
                batch = at_group * group + k
                owner = batch // owned

                @pl.when((section == last) & (owner != last))
                def _():
                    pltpu.make_async_remote_copy(
                        src_ref=left.at[at_group, pl.ds(k * rows, rows), columns],
                        dst_ref=out.at[lax.rem(batch, owned), :, columns],
                        send_sem=send_sem.at[at_group],
                        recv_sem=out_sem.at[lax.rem(batch, owned)],
                        device_id={"section": owner},
                        device_id_type=MESH,
                    ).start()

                @pl.when((section == last) & (owner == last))
                def _():
                    pltpu.make_async_copy(
                        left.at[at_group, pl.ds(k * rows, rows), columns],
                        out.at[lax.rem(batch, owned), :, columns],
                        out_sem.at[lax.rem(batch, owned)],
                    ).start()

        return carry

    lax.fori_loop(0, groups, one_group, 0)

    for slot in range(owned):
        pltpu.make_async_copy(out.at[slot], out.at[slot], out_sem.at[slot]).wait()

    for batch in range(batches):
        sent = left.at[batch // group, pl.ds(batch % group * rows, rows), :]

        @pl.when((section < last) | (batch // owned != last))
        def _():
            pltpu.make_async_copy(sent, sent, send_sem.at[batch // group]).wait()

    others = all_stats.at[pl.ds(0, shards - 1)]
    pltpu.make_async_copy(others, others, stat_send).wait()
    pltpu.make_async_copy(others, others, stat_recv).wait()
    total = all_stats[0]
    for at in range(1, shards):
        total = total + all_stats[at]
    tokens = jnp.float32(batches * rows * shards)
    fractions = total[0:1, :] / (tokens * jnp.float32(picks))
    mean_probs = total[1:2, :] / tokens
    loss[0] = jnp.float32(experts) * jnp.sum(fractions * mean_probs)


def per_device(hidden_in, norm_gain, router_weight, expert_scale, mix_weight, routes):
    sections = lax.axis_size("section")
    shards = lax.axis_size("dp")
    batches, rows, width = hidden_in.shape
    experts = router_weight.shape[2]
    picks = routes.shape[3]
    group = 1
    groups, tall = batches // group, group * rows
    chunk = 512
    pieces = width // chunk
    anywhere = pl.BlockSpec(memory_space=pl.ANY)
    return pl.pallas_call(
        functools.partial(relay, sections, shards, chunk, group),
        out_shape=(
            jax.ShapeDtypeStruct((batches // sections, rows, width), jnp.bfloat16),
            jax.ShapeDtypeStruct((1,), jnp.float32),
        ),
        in_specs=[anywhere] * 6,
        out_specs=(anywhere, pl.BlockSpec(memory_space=pltpu.SMEM)),
        scratch_shapes=[
            pltpu.VMEM((groups, tall, width), jnp.bfloat16),
            pltpu.VMEM((groups, tall, width), jnp.bfloat16),
            pltpu.VMEM((width, width), jnp.bfloat16),
            pltpu.VMEM((experts, width), jnp.bfloat16),
            pltpu.VMEM((experts, width), jnp.bfloat16),
            pltpu.VMEM((1, width), jnp.bfloat16),
            pltpu.VMEM((batches, picks, rows), jnp.int32),
            pltpu.VMEM((tall, width), jnp.bfloat16),
            pltpu.VMEM((tall, width), jnp.bfloat16),
            pltpu.VMEM((8, 128), jnp.float32),
            pltpu.VMEM((shards, 8, 128), jnp.float32),
            pltpu.SemaphoreType.DMA((groups,)),
            pltpu.SemaphoreType.DMA((groups,)),
            pltpu.SemaphoreType.DMA((batches // sections,)),
            pltpu.SemaphoreType.DMA((pieces,)),
            pltpu.SemaphoreType.DMA((4,)),
            pltpu.SemaphoreType.DMA,
            pltpu.SemaphoreType.DMA,
        ],
        compiler_params=pltpu.CompilerParams(collective_id=0, has_side_effects=True),
    )(
        hidden_in,
        norm_gain,
        jnp.transpose(router_weight[0]),
        expert_scale,
        mix_weight,
        jnp.swapaxes(routes, 2, 3),
    )


def solution(mesh):
    placed = (
        P(None, "dp", None),
        P("section", None),
        P("section", None, None),
        P("section", None, None),
        P("section", None, None),
        P("section", None, "dp", None),
    )
    return jax.shard_map(
        per_device,
        mesh=mesh,
        in_specs=placed,
        out_specs=(P("section", "dp", None), P("section")),
        check_vma=False,
    )
```
